32 devices in a mesh: kx: 4 (over y, x), ky: 8 (over z, core).
Axes of the slice: x: 2, y: 2, z: 4, core: 2. Of those that a mesh axis runs over, the one named last changes fastest.
Arguments:
- wannier: bfloat16 [16, 64, 64, 128], P('kx', 'ky'), may hold values from -0.5 to 0.5
- coupling: bfloat16 [3, 16, 64, 6, 64, 128], P(None, 'kx', 'ky'), may hold values from -6 to 6
- kq_map: int32 [3, 1024], replicated, may hold values from 0 to 1023, as said below
Outputs:
- rotated: bfloat16 [3, 16, 64, 6, 64, 128], P(None, 'kx', 'ky')
The draws below stay inside these ranges and needn't reach their ends.
Inputs may be any that keep to these rules, and one draw needn't show every extreme that they name: For every q there are offsets a and b with kq_map[q, x * 64 + y] = ((x + a) mod 16) * 64 + (y + b) mod 64.
All inputs are finite; a program needn't handle non-finite values.
Results may differ from the reference program's by a relative error of at most 0.0049.
Values may be sent and summed in bfloat16 or wider, within the bound.
A program may use at most 192 MiB of HBM per device.

```python
import jax
import jax.numpy as jnp

NB = 64
MODES = 6
Q = 3
KX_DEV = 4
KY_DEV = 8
NX = 16
NY = 64


def draw_kq_map(key, part):
    blocks_x = jax.random.randint(jax.random.fold_in(key, 11), (Q,), 0, NX // KX_DEV)
    blocks_x = blocks_x.at[0].set(NX // KX_DEV - 1)
    blocks_x = blocks_x.at[1].set(NX // KX_DEV // 2)
    blocks_y = jax.random.randint(jax.random.fold_in(key, 23), (Q,), 0, NY // KY_DEV)
    blocks_y = blocks_y.at[0].set(NY // KY_DEV - 1)
    blocks_y = blocks_y.at[1].set(NY // KY_DEV // 2)
    inner_x = jax.random.randint(jax.random.fold_in(key, 37), (Q,), 1, KX_DEV)
    inner_y = jax.random.randint(jax.random.fold_in(key, 41), (Q,), 1, KY_DEV)
    shift_x = blocks_x * KX_DEV + inner_x
    shift_y = blocks_y * KY_DEV + inner_y
    grid_x = jnp.arange(NX, dtype=jnp.int32)[None, :, None]
    grid_y = jnp.arange(NY, dtype=jnp.int32)[None, None, :]
    mapped = (grid_x + shift_x[:, None, None]) % NX * NY + (grid_y + shift_y[:, None, None]) % NY
    return mapped.reshape(Q, NX * NY).astype(jnp.int32)


def levels(own_key, dims, pieces, low, largest):
    def one(position, blocks):
        steps = jax.random.uniform(jax.random.fold_in(jax.random.fold_in(own_key, 6), position), (blocks,), jnp.float32, low / len(pieces), largest / len(pieces))
        return jnp.repeat(jnp.exp(steps), dims[position] // blocks).reshape((-1,) + (1,) * (len(dims) - position - 1))

    gain = one(*pieces[0])
    for cut in pieces[1:]:
        gain = gain * one(*cut)
    return gain


def centred(own_key, shape, spread, bound, cuts=(), kind=jnp.bfloat16):
    drawn = jax.random.normal(own_key, shape, jnp.float32) * spread
    if len(cuts) > 0:
        drawn = levels(own_key, shape, cuts, -0.22, 0.18) * drawn
    return jnp.clip(drawn, min=-bound, max=bound).astype(kind)


def setup_inputs(seed: int = 0) -> dict:
    key_list = jax.random.split(jax.random.key(seed), 4)
    return {
        "wannier": centred(key_list[0], (NX, NY, NB, 2 * NB), (2 * NB) ** -0.5, 0.5, ((0, 4), (1, 8))),
        "coupling": centred(key_list[1], (Q, NX, NY, MODES, NB, 2 * NB), 1.0, 6.0, ((1, 4), (2, 8))),
        "kq_map": draw_kq_map(jax.random.fold_in(key_list[3], 71), 0),
    }


def right_factor(matrix):
    half_width = matrix.shape[-1] // 2
    lower_half = jnp.concatenate([-matrix[..., half_width:], matrix[..., :half_width]], axis=-1)
    return jnp.concatenate([matrix, lower_half], axis=-2)


def rotate(block_g, factor, partner):
    half_width = partner.shape[-1] // 2
    half_turn = jnp.einsum("xymac,xycd->xymad", block_g.astype(jnp.float32), factor.astype(jnp.float32)).astype(jnp.bfloat16)
    stacked = jnp.concatenate([half_turn, jnp.concatenate([half_turn[..., half_width:], -half_turn[..., :half_width]], axis=-1)], axis=-2)
    partner_rows = jnp.concatenate([partner[..., :half_width], partner[..., half_width:]], axis=-2)
    return jnp.einsum("xyca,xymcd->xymad", partner_rows.astype(jnp.float32), stacked.astype(jnp.float32)).astype(jnp.bfloat16)


def reference(wannier, coupling, kq_map):
    factor = right_factor(wannier)
    flattened = wannier.reshape(NX * NY, NB, 2 * NB)
    results = []
    for qpoint in range(Q):
        partner = flattened[kq_map[qpoint]].reshape(NX, NY, NB, 2 * NB)
        results.append(rotate(coupling[qpoint], factor, partner))
    return jnp.stack(results, axis=0)
```

```python
import functools

import jax
import jax.numpy as jnp
from jax import lax
from jax.experimental import pallas as pl
from jax.experimental.pallas import tpu as pltpu
from jax.sharding import PartitionSpec as P

MESH = pl.DeviceIdType.MESH
CORES = 2
SLAB = 16


def exchange_kernel(plan, map_ref, wannier_ref, partner_ref, *scratch):
    count_x, planes, rows_x, cols_y, qpoints, parts, waves = plan
    mates = count_x * CORES
    total_x, total_y, blocks = count_x * rows_x, planes * CORES * cols_y, planes * CORES
    gathered, staged = scratch[:waves], scratch[waves : 2 * waves]
    spread_send, spread_recv, spread_self, chain_send, chain_recv, pick_send, pick_recv, pick_self = scratch[2 * waves :]

    here_x, here_y = lax.axis_index("kx"), lax.axis_index("ky")
    plane, core = here_y // CORES, here_y % CORES
    mate = here_x * CORES + core

    def device_of(other):
        return (other // CORES, plane * CORES + other % CORES)

    def part_of(other):
        return other // cols_y if parts > 1 else 0

    def slab(part, wave):
        return pl.ds(pl.multiple_of((part * waves + wave) * SLAB, SLAB), SLAB)

    def spread(wave, step):
        other = (mate + step) % mates
        source = wannier_ref.at[:, other % cols_y, slab(part_of(other), wave), :]
        target = gathered[wave].at[here_y, pl.ds(here_x * rows_x, rows_x)]
        if step == 0:
            return pltpu.make_async_copy(source, target, spread_self.at[wave])
        return pltpu.make_async_remote_copy(
            source, target, spread_send.at[wave, step], spread_recv.at[wave, step], device_of(other), MESH
        )

    def chain(wave, origin, distance, side):
        block = gathered[wave].at[pl.ds(origin * CORES, CORES)]
        target = (here_x, here_y + (CORES if side else -CORES))
        return pltpu.make_async_remote_copy(
            block, block, chain_send.at[wave, distance, side], chain_recv.at[wave, origin], target, MESH
        )

    def pick(wave, step):
        source = staged[wave].at[step]
        target = partner_ref.at[mate % cols_y, :, :, slab(part_of(mate), wave), :]
        if step == 0:
            return pltpu.make_async_copy(source, target, pick_self.at[wave])
        return pltpu.make_async_remote_copy(
            source, target, pick_send.at[wave, step], pick_recv.at[wave, step], device_of((mate + step) % mates), MESH
        )

    def stage(wave):
        kind = mate % cols_y

        def one(step, carry):
            other = (mate + step) % mates
            for q in range(qpoints):
                shift_x, shift_y = map_ref[q, 0] // total_y, map_ref[q, 0] % total_y
                block = (plane * CORES + other % CORES + (shift_y - kind + cols_y - 1) // cols_y) % blocks
                for row in range(rows_x):
                    staged[wave][step, q, row] = gathered[wave][block, (other // CORES * rows_x + shift_x + row) % total_x]
            return carry

        lax.fori_loop(0, mates, one, 0)

    has_left, has_right = plane > 0, plane < planes - 1

    barrier = pltpu.get_barrier_semaphore()
    for step in range(1, mates):
        pl.semaphore_signal(barrier, inc=1, device_id=device_of((mate + step) % mates), device_id_type=MESH)

    @pl.when(has_left)
    def _():
        pl.semaphore_signal(barrier, inc=1, device_id=(here_x, here_y - CORES), device_id_type=MESH)

    @pl.when(has_right)
    def _():
        pl.semaphore_signal(barrier, inc=1, device_id=(here_x, here_y + CORES), device_id_type=MESH)

    pl.semaphore_wait(barrier, mates - 1 + has_left.astype(jnp.int32) + has_right.astype(jnp.int32))

    for wave in range(waves):
        for step in range(mates):
            spread(wave, step).start()

    def send(wave, origin, distance, side):
        @pl.when(has_right if side else has_left)
        def _():
            chain(wave, origin, distance, side).start()

    for tick in range(waves + planes):
        if tick < waves:
            spread(tick, 0).wait()
            for step in range(1, mates):
                spread(tick, step).wait_recv()
            for side in range(2):
                send(tick, plane, 0, side)
        for distance in range(1, planes):
            wave = tick - distance
            if not 0 <= wave < waves:
                continue

            @pl.when(plane + distance < planes)
            def _():
                chain(wave, plane + distance, distance, 0).wait_recv()
                if distance < planes - 1:
                    send(wave, plane + distance, distance, 0)

            @pl.when(plane >= distance)
            def _():
                chain(wave, plane - distance, distance, 1).wait_recv()
                if distance < planes - 1:
                    send(wave, plane - distance, distance, 1)

        wave = tick - planes + 1
        if 0 <= wave < waves:
            stage(wave)
            for step in range(mates):
                pick(wave, step).start()

    for wave in range(waves):
        for step in range(1, mates):
            spread(wave, step).wait_send()
        for distance in range(planes - 1):

            @pl.when((plane + distance < planes) & has_left)
            def _():
                chain(wave, plane + distance, distance, 0).wait_send()

            @pl.when((plane >= distance) & has_right)
            def _():
                chain(wave, plane - distance, distance, 1).wait_send()

        pick(wave, 0).wait()
        for step in range(1, mates):
            pick(wave, step).wait()


def exchange(kq_map, wannier, count_x, count_y):
    rows_x, cols_y, bands, width = wannier.shape
    qpoints = kq_map.shape[0]
    planes, mates = count_y // CORES, count_x * CORES
    parts = mates // cols_y
    assert parts * cols_y == mates and planes * CORES == count_y
    waves = bands // (parts * SLAB)
    plan = (count_x, planes, rows_x, cols_y, qpoints, parts, waves)
    dma = pltpu.SemaphoreType.DMA
    return pl.pallas_call(
        functools.partial(exchange_kernel, plan),
        out_shape=jax.ShapeDtypeStruct((cols_y, qpoints, rows_x, bands, width), wannier.dtype),
        grid=(1,),
        in_specs=[
            pl.BlockSpec((qpoints, 128), lambda i: (0, 0), memory_space=pltpu.SMEM),
            pl.BlockSpec(memory_space=pl.ANY),
        ],
        out_specs=pl.BlockSpec(memory_space=pl.ANY),
        scratch_shapes=[pltpu.VMEM((count_y, count_x * rows_x, SLAB, width), wannier.dtype)] * waves
        + [pltpu.VMEM((mates, qpoints, rows_x, SLAB, width), wannier.dtype)] * waves
        + [
            dma((waves, mates)),
            dma((waves, mates)),
            dma((waves,)),
            dma((waves, planes, 2)),
            dma((waves, planes)),
            dma((waves, mates)),
            dma((waves, mates)),
            dma((waves,)),
        ],
        compiler_params=pltpu.CompilerParams(collective_id=0, has_side_effects=True),
    )(kq_map, wannier)


def rotate_kernel(column_ref, coupling_ref, wannier_ref, *refs):
    partner_refs, out_ref = refs[:-1], refs[-1]
    qpoints, rows, _, modes, bands, width = coupling_ref.shape
    half = width // 2
    for first in range(0, rows, 2):
        turned = []
        for row in (first, first + 1):
            real, imag = wannier_ref[row, 0, :, :half], wannier_ref[row, 0, :, half:]
            factor = jnp.concatenate(
                [jnp.concatenate([real, imag], axis=1), jnp.concatenate([-imag, real], axis=1)], axis=0
            )
            blank = jnp.zeros_like(factor)
            pair_factor = jnp.concatenate(
                [jnp.concatenate([factor, blank], axis=1), jnp.concatenate([blank, factor], axis=1)], axis=0
            )
            blocks = coupling_ref[:, row, 0].reshape(qpoints * modes // 2, 2, bands, width)
            pairs = jnp.concatenate([blocks[:, 0].reshape(-1, width), blocks[:, 1].reshape(-1, width)], axis=1)
            turned.append(jnp.dot(pairs, pair_factor, preferred_element_type=jnp.float32).astype(jnp.bfloat16))
        for q in range(qpoints):
            stacked, partner_rows = [], []
            for side, row in enumerate((first, first + 1)):
                parts = []
                for mode in range(modes):
                    pair, lane = divmod(q * modes + mode, 2)
                    own = turned[side][pair * bands : (pair + 1) * bands, lane * width : (lane + 1) * width]
                    swapped = jnp.concatenate([own[:, half:], -own[:, :half]], axis=1)
                    parts.append(jnp.concatenate([own, swapped], axis=0))
                stacked.append(jnp.concatenate(parts, axis=1))
                partner = partner_refs[q][0, 0, row]
                column = jnp.concatenate([partner[:, :half], partner[:, half:]], axis=0)
                blank = jnp.zeros_like(column)
                partner_rows.append(jnp.concatenate([blank, column] if side else [column, blank], axis=1))
            rotated = lax.dot_general(
                jnp.concatenate(partner_rows, axis=0),
                jnp.concatenate(stacked, axis=0),
                (((0,), (0,)), ((), ())),
                preferred_element_type=jnp.float32,
            ).astype(jnp.bfloat16)
            for side, row in enumerate((first, first + 1)):
                for mode in range(modes):
                    out_ref[q, row, 0, mode] = rotated[side * bands : (side + 1) * bands, mode * width : (mode + 1) * width]


def rotate(columns, coupling, wannier, partner):
    qpoints, rows, cols, modes, bands, width = coupling.shape
    all_modes = pl.BlockSpec((qpoints, rows, 1, modes, bands, width), lambda p, c: (0, 0, p, 0, 0, 0))

    def partner_spec(q):
        return pl.BlockSpec((1, 1, rows, bands, width), lambda p, c: ((p + c[q]) % cols, q, 0, 0, 0))

    return pl.pallas_call(
        rotate_kernel,
        grid_spec=pltpu.PrefetchScalarGridSpec(
            num_scalar_prefetch=1,
            grid=(cols,),
            in_specs=[all_modes, pl.BlockSpec((rows, 1, bands, width), lambda p, c: (0, p, 0, 0))]
            + [partner_spec(q) for q in range(qpoints)],
            out_specs=all_modes,
        ),
        out_shape=jax.ShapeDtypeStruct(coupling.shape, coupling.dtype),
    )(columns, coupling, wannier, *[partner] * qpoints)


def per_device(wannier, coupling, kq_map):
    count_x, count_y = lax.axis_size("kx"), lax.axis_size("ky")
    partner = exchange(kq_map, wannier, count_x, count_y)
    return rotate(kq_map[:, 0] % wannier.shape[1], coupling, wannier, partner)


def solution(mesh):
    in_specs = (P("kx", "ky", None, None), P(None, "kx", "ky", None, None, None), P())
    out_specs = P(None, "kx", "ky", None, None, None)
    return jax.shard_map(
        per_device, mesh=mesh, in_specs=in_specs, out_specs=out_specs, check_vma=False
    )
```

```python
import functools

import jax
import jax.numpy as jnp
from jax import lax
from jax.experimental import pallas as pl
from jax.experimental.pallas import tpu as pltpu
from jax.sharding import PartitionSpec as P

MESH = pl.DeviceIdType.MESH
CORES = 2
SLAB = 16
UNROLL = 8
DEPTH = 4


def turn_point(coupling, wannier, out):
    qpoints, modes, bands, width = coupling.shape
    half = width // 2
    real, imag = wannier[:, :half], wannier[:, half:]
    plain = jnp.concatenate([jnp.concatenate([real, imag], axis=1), jnp.concatenate([-imag, real], axis=1)], axis=0)
    swapped = jnp.concatenate([jnp.concatenate([imag, -real], axis=1), jnp.concatenate([real, imag], axis=1)], axis=0)
    blank = jnp.zeros_like(plain)
    blocks = coupling[...].reshape(qpoints * modes // 2, 2, bands, width)
    pairs = jnp.concatenate([blocks[:, 0].reshape(-1, width), blocks[:, 1].reshape(-1, width)], axis=1)
    for side, factor in enumerate((plain, swapped)):
        pair_factor = jnp.concatenate(
            [jnp.concatenate([factor, blank], axis=1), jnp.concatenate([blank, factor], axis=1)], axis=0
        )
        turned = jnp.dot(pairs, pair_factor, preferred_element_type=jnp.float32).astype(out.dtype)
        for index in range(qpoints * modes):
            pair, lane = divmod(index, 2)
            q, mode = divmod(index, modes)
            out[q, side * bands : (side + 1) * bands, mode * width : (mode + 1) * width] = turned[
                pair * bands : (pair + 1) * bands, lane * width : (lane + 1) * width
            ]


def exchange_kernel(plan, map_hbm, wannier_hbm, coupling_ref, partner_ref, turned_ref, *scratch):
    count_x, planes, rows_x, cols_y, qpoints, parts, waves = plan
    mates = count_x * CORES
    total_x, total_y, blocks = count_x * rows_x, planes * CORES * cols_y, planes * CORES
    gathered, staged, arrived = (scratch[part * waves : (part + 1) * waves] for part in range(3))
    spread_send, spread_recv, spread_self, chain_send, chain_recv, pick_send, pick_recv = scratch[3 * waves :][:7]
    map_ref, map_sem, wannier_ref, wannier_sem, held_in, in_sem = scratch[3 * waves + 7 :]
    points, depth = rows_x * cols_y, held_in.shape[0]

    here_x, here_y = lax.axis_index("kx"), lax.axis_index("ky")
    plane, core = here_y // CORES, here_y % CORES
    mate = here_x * CORES + core

    def device_of(other):
        return (other // CORES, plane * CORES + other % CORES)

    def part_of(other):
        return other // cols_y if parts > 1 else 0

    def slab(part, wave):
        return pl.ds(pl.multiple_of((part * waves + wave) * SLAB, SLAB), SLAB)

    def spread(wave, step):
        other = (mate + step) % mates
        window = (slice(None), other % cols_y, slab(part_of(other), wave), slice(None))
        target = gathered[wave].at[here_y, pl.ds(here_x * rows_x, rows_x)]
        if step == 0:
            return pltpu.make_async_copy(wannier_hbm.at[window], target, spread_self.at[wave])
        source = wannier_ref.at[window]
        return pltpu.make_async_remote_copy(
            source, target, spread_send.at[wave, step], spread_recv.at[wave, step], device_of(other), MESH
        )

    def chain(wave, origin, distance, side):
        block = gathered[wave].at[pl.ds(origin * CORES, CORES)]
        target = (here_x, here_y + (CORES if side else -CORES))
        return pltpu.make_async_remote_copy(
            block, block, chain_send.at[wave, distance, side], chain_recv.at[wave, origin], target, MESH
        )

    def pick(wave, step):
        source = staged[wave].at[step]
        target = arrived[wave].at[mate]
        return pltpu.make_async_remote_copy(
            source, target, pick_send.at[wave, step], pick_recv.at[wave, step], device_of((mate + step) % mates), MESH
        )

    def stage(wave):
        kind = mate % cols_y

        def one(step, carry):
            other = (mate + step) % mates
            for q in range(qpoints):
                shift_x, shift_y = map_ref[q, 0] // total_y, map_ref[q, 0] % total_y
                block = (plane * CORES + other % CORES + (shift_y - kind + cols_y - 1) // cols_y) % blocks
                for row in range(rows_x):
                    staged[wave][step, q, row] = gathered[wave][block, (other // CORES * rows_x + shift_x + row) % total_x]
            return carry

        lax.fori_loop(0, mates, one, 0)
        for q in range(qpoints):
            for row in range(rows_x):
                arrived[wave][mate, q, row] = staged[wave][0, q, row]

    def settle(wave):
        for step in range(1, mates):
            pick(wave, step).wait_recv()

        def one(col, carry):
            for q in range(qpoints):
                for part in range(parts):
                    source = part * cols_y + (col + map_ref[q, 0]) % cols_y
                    for row in range(rows_x):
                        partner_ref[col, q, row, slab(part, wave), :] = arrived[wave][source, q, row]
            return carry

        lax.fori_loop(0, cols_y, one, 0)

    def fetch(point):
        slot = point % depth
        return pltpu.make_async_copy(coupling_ref.at[:, point % rows_x, point // rows_x], held_in.at[slot], in_sem.at[slot])

    def turn(point, carry):
        slot = point % depth
        fetch(point).wait()
        turn_point(held_in.at[slot], wannier_ref[point % rows_x, point // rows_x], turned_ref.at[point // rows_x, point % rows_x])

        @pl.when(point + depth < points)
        def _():
            fetch(point + depth).start()

        return carry

    turned = 0

    def fill(count):
        nonlocal turned
        last = min(points, turned + count)
        if last > turned:
            lax.fori_loop(turned, last, turn, 0)
        turned = last

    map_copy = pltpu.make_async_copy(map_hbm, map_ref, map_sem)
    wannier_copy = pltpu.make_async_copy(wannier_hbm, wannier_ref, wannier_sem)
    wannier_copy.start()
    map_copy.start()
    for point in range(depth):
        fetch(point).start()

    has_left, has_right = plane > 0, plane < planes - 1

    barrier = pltpu.get_barrier_semaphore()
    for step in range(1, mates):
        pl.semaphore_signal(barrier, inc=1, device_id=device_of((mate + step) % mates), device_id_type=MESH)

    @pl.when(has_left)
    def _():
        pl.semaphore_signal(barrier, inc=1, device_id=(here_x, here_y - CORES), device_id_type=MESH)

    @pl.when(has_right)
    def _():
        pl.semaphore_signal(barrier, inc=1, device_id=(here_x, here_y + CORES), device_id_type=MESH)

    pl.semaphore_wait(barrier, mates - 1 + has_left.astype(jnp.int32) + has_right.astype(jnp.int32))

    wannier_copy.wait()
    for wave in range(waves):
        for step in range(mates):
            spread(wave, step).start()
    map_copy.wait()

    def send(wave, origin, distance, side):
        @pl.when(has_right if side else has_left)
        def _():
            chain(wave, origin, distance, side).start()

    def launch(wave):
        spread(wave, 0).wait()
        for step in range(1, mates):
            spread(wave, step).wait_recv()
        for side in range(2):
            send(wave, plane, 0, side)

    for wave in range(min(2, waves)):
        fill(2)
        launch(wave)

    for tick in range(1, waves + planes - 1):
        for distance in reversed(range(1, planes)):
            wave = tick - distance
            if not 0 <= wave < waves:
                continue
            fill(2)

            @pl.when(plane + distance < planes)
            def _():
                chain(wave, plane + distance, distance, 0).wait_recv()
                if distance < planes - 1:
                    send(wave, plane + distance, distance, 0)

            @pl.when(plane >= distance)
            def _():
                chain(wave, plane - distance, distance, 1).wait_recv()
                if distance < planes - 1:
                    send(wave, plane - distance, distance, 1)

        if tick + 1 < waves:
            launch(tick + 1)
        wave = tick - planes + 1
        if 0 <= wave < waves:
            stage(wave)
            for step in range(1, mates):
                pick(wave, step).start()
            if wave > 0:
                settle(wave - 1)

    fill(points)
    settle(waves - 1)

    for wave in range(waves):
        for step in range(1, mates):
            spread(wave, step).wait_send()
        for distance in range(planes - 1):

            @pl.when((plane + distance < planes) & has_left)
            def _():
                chain(wave, plane + distance, distance, 0).wait_send()

            @pl.when((plane >= distance) & has_right)
            def _():
                chain(wave, plane - distance, distance, 1).wait_send()

        for step in range(1, mates):
            pick(wave, step).wait_send()


def exchange(kq_map, wannier, coupling, count_x, count_y):
    rows_x, cols_y, bands, width = wannier.shape
    qpoints, modes = coupling.shape[0], coupling.shape[3]
    planes, mates = count_y // CORES, count_x * CORES
    parts = mates // cols_y
    assert parts * cols_y == mates and planes * CORES == count_y
    waves = bands // (parts * SLAB)
    plan = (count_x, planes, rows_x, cols_y, qpoints, parts, waves)
    dma = pltpu.SemaphoreType.DMA
    hbm, vmem = pl.BlockSpec(memory_space=pltpu.HBM), pl.BlockSpec(memory_space=pltpu.VMEM)
    kind = coupling.dtype
    return pl.pallas_call(
        functools.partial(exchange_kernel, plan),
        out_shape=[
            jax.ShapeDtypeStruct((cols_y, qpoints, rows_x, bands, width), kind),
            jax.ShapeDtypeStruct((cols_y, rows_x, qpoints, 2 * bands, modes * width), kind),
        ],
        in_specs=[hbm, hbm, hbm],
        out_specs=[vmem, vmem],
        scratch_shapes=[pltpu.VMEM((count_y, count_x * rows_x, SLAB, width), kind)] * waves
        + [pltpu.VMEM((mates, qpoints, rows_x, SLAB, width), kind)] * (2 * waves)
        + [
            dma((waves, mates)),
            dma((waves, mates)),
            dma((waves,)),
            dma((waves, planes, 2)),
            dma((waves, planes)),
            dma((waves, mates)),
            dma((waves, mates)),
            pltpu.SMEM(kq_map.shape, jnp.int32),
            dma(()),
            pltpu.VMEM(wannier.shape, kind),
            dma(()),
            pltpu.VMEM((DEPTH, qpoints, modes, bands, width), kind),
            dma((DEPTH,)),
        ],
        compiler_params=pltpu.CompilerParams(collective_id=0, has_side_effects=True, vmem_limit_bytes=16 << 20),
    )(*[pltpu.with_memory_space_constraint(a, pltpu.HBM) for a in (kq_map, wannier, coupling)])


def rotate_kernel(partner_ref, turned_ref, out_hbm, out_ref, out_sem):
    cols, qpoints, rows, modes, bands, width = out_ref.shape
    half = width // 2

    def flush(col):
        return pltpu.make_async_copy(out_ref.at[col], out_hbm.at[:, :, col], out_sem.at[col])

    def one(col, carry):
        for q in range(qpoints):
            for first in range(0, rows, 2):
                partner_rows = []
                for side, row in enumerate((first, first + 1)):
                    partner = partner_ref[col, q, row]
                    column = jnp.concatenate([partner[:, :half], partner[:, half:]], axis=0)
                    blank = jnp.zeros_like(column)
                    partner_rows.append(jnp.concatenate([blank, column] if side else [column, blank], axis=1))
                rotated = lax.dot_general(
                    jnp.concatenate(partner_rows, axis=0),
                    jnp.concatenate([turned_ref[col, row, q] for row in (first, first + 1)], axis=0),
                    (((0,), (0,)), ((), ())),
                    preferred_element_type=jnp.float32,
                ).astype(out_ref.dtype)
                for side, row in enumerate((first, first + 1)):
                    for mode in range(modes):
                        out_ref[col, q, row, mode] = rotated[side * bands : (side + 1) * bands, mode * width : (mode + 1) * width]
        flush(col).start()
        return carry

    lax.fori_loop(0, cols, one, 0, unroll=UNROLL)
    for col in range(cols):
        flush(col).wait()


def rotate(turned, partner):
    cols, qpoints, rows, bands, width = partner.shape
    modes = turned.shape[-1] // width
    hbm, vmem = pl.BlockSpec(memory_space=pltpu.HBM), pl.BlockSpec(memory_space=pltpu.VMEM)
    return pl.pallas_call(
        rotate_kernel,
        in_specs=[vmem, vmem],
        out_specs=hbm,
        out_shape=jax.ShapeDtypeStruct((qpoints, rows, cols, modes, bands, width), turned.dtype),
        scratch_shapes=[
            pltpu.VMEM((cols, qpoints, rows, modes, bands, width), turned.dtype),
            pltpu.SemaphoreType.DMA((cols,)),
        ],
        compiler_params=pltpu.CompilerParams(vmem_limit_bytes=16 << 20),
    )(partner, turned)


def per_device(wannier, coupling, kq_map):
    partner, turned = exchange(kq_map, wannier, coupling, lax.axis_size("kx"), lax.axis_size("ky"))
    return rotate(turned, partner)


def solution(mesh):
    in_specs = (P("kx", "ky", None, None), P(None, "kx", "ky", None, None, None), P())
    out_specs = P(None, "kx", "ky", None, None, None)
    return jax.shard_map(
        per_device, mesh=mesh, in_specs=in_specs, out_specs=out_specs, check_vma=False
    )
```

```python
import functools

import jax
import jax.numpy as jnp
from jax import lax
from jax.experimental import pallas as pl
from jax.experimental.pallas import tpu as pltpu
from jax.sharding import PartitionSpec as P

MESH = pl.DeviceIdType.MESH
CORES = 2
SLAB = 16
SLOTS = 4
UNROLL = 8
DEPTH = 4


def turn_point(coupling, wannier, out):
    qpoints, modes, bands, width = coupling.shape
    half = width // 2
    real, imag = wannier[:, :half], wannier[:, half:]
    plain = jnp.concatenate([jnp.concatenate([real, imag], axis=1), jnp.concatenate([-imag, real], axis=1)], axis=0)
    swapped = jnp.concatenate([jnp.concatenate([imag, -real], axis=1), jnp.concatenate([real, imag], axis=1)], axis=0)
    blank = jnp.zeros_like(plain)
    blocks = coupling[...].reshape(qpoints * modes // 2, 2, bands, width)
    pairs = jnp.concatenate([blocks[:, 0].reshape(-1, width), blocks[:, 1].reshape(-1, width)], axis=1)
    for side, factor in enumerate((plain, swapped)):
        pair_factor = jnp.concatenate(
            [jnp.concatenate([factor, blank], axis=1), jnp.concatenate([blank, factor], axis=1)], axis=0
        )
        turned = jnp.dot(pairs, pair_factor, preferred_element_type=jnp.float32).astype(out.dtype)
        for index in range(qpoints * modes):
            pair, lane = divmod(index, 2)
            q, mode = divmod(index, modes)
            out[q, side * bands : (side + 1) * bands, mode * width : (mode + 1) * width] = turned[
                pair * bands : (pair + 1) * bands, lane * width : (lane + 1) * width
            ]


def wrap(value, size):
    return value & (size - 1) if size & (size - 1) == 0 else lax.rem(value, size)


def exchange_kernel(plan, map_hbm, wannier_hbm, coupling_ref, partner_ref, turned_ref, *scratch):
    few, count_x, planes, rows_x, cols_y, qpoints, parts, slabs = plan
    waves = len(slabs)
    mates = count_x * CORES
    total_x, total_y, blocks = count_x * rows_x, planes * CORES * cols_y, planes * CORES
    gathered, far, chosen, staged, arrived = (scratch[part * waves : (part + 1) * waves] for part in range(5))
    spread_send, spread_recv, spread_self, chain_send, chain_recv, pick_send, pick_recv = scratch[5 * waves :][:7]
    map_ref, map_sem, wannier_ref, wannier_sem, held_in, in_sem, place_ref, take_ref, shift_ref = scratch[5 * waves + 7 :]
    points, depth = rows_x * cols_y, held_in.shape[0]

    here_x, here_y = lax.axis_index("kx"), lax.axis_index("ky")
    plane, core = here_y // CORES, here_y % CORES
    mate = here_x * CORES + core

    def device_of(other):
        return (other // CORES, plane * CORES + other % CORES)

    def part_of(other):
        return other // cols_y if parts > 1 else 0

    def slab(part, wave):
        start, size = slabs[wave]
        return pl.ds(pl.multiple_of(part * (slabs[-1][0] + slabs[-1][1]) + start, size), size)

    def spread(wave, step):
        other = (mate + step) % mates
        window = (slice(None), other % cols_y, slab(part_of(other), wave), slice(None))
        target = gathered[wave].at[core if few else here_y, pl.ds(here_x * rows_x, rows_x)]
        if step == 0:
            return pltpu.make_async_copy(wannier_hbm.at[window], target, spread_self.at[wave])
        source = wannier_ref.at[window]
        return pltpu.make_async_remote_copy(
            source, target, spread_send.at[wave, step], spread_recv.at[wave, step], device_of(other), MESH
        )

    def chain(wave, origin, distance, side):
        block = gathered[wave].at[pl.ds(origin * CORES, CORES)]
        target = (here_x, here_y + (CORES if side else -CORES))
        return pltpu.make_async_remote_copy(
            block, block, chain_send.at[wave, distance, side], chain_recv.at[wave, origin], target, MESH
        )

    inner = (plane > 0) & (plane < planes - 1)
    end = jnp.where(inner, (plane - 1) * (planes - 1), plane)

    def hop(wave, kind):
        near_pair, last_pair = pl.ds(0, CORES), pl.ds(CORES, CORES)
        other_inner, next_inner, next_end = planes - 1 - plane, 1 + plane // (planes - 1), (plane - 1) * (planes - 1)
        source, target, index, to = (
            (gathered[wave].at[near_pair], gathered[wave].at[last_pair], 0, other_inner),
            (gathered[wave].at[near_pair], far[wave].at[near_pair], 1, next_inner),
            (far[wave].at[near_pair], far[wave].at[last_pair], 2, other_inner),
            (chosen[wave].at[near_pair], gathered[wave].at[last_pair], 0, next_end),
            (chosen[wave].at[last_pair], far[wave].at[near_pair], 1, next_end),
        )[kind]
        return pltpu.make_async_remote_copy(
            source, target, chain_send.at[wave, kind], chain_recv.at[wave, index], (here_x, to * CORES + core), MESH
        )

    def first_block(q):
        return (map_ref[q, 0] % total_y - mate % cols_y + cols_y - 1) // cols_y % blocks

    def assign():
        firsts = [first_block(q) for q in range(qpoints)]
        free, slots, takes = 0, [], list(range(SLOTS))
        for index in range(blocks - CORES):
            away = index // CORES + 1
            block = jnp.where(end == 0, away, end - away) * CORES + index % CORES
            needed = False
            for first in firsts:
                ahead = (block - end * CORES - first) % blocks
                needed = needed | (ahead == 0) | (ahead == 1)
            slot = jnp.maximum(free, index - (blocks - CORES - SLOTS))
            free = jnp.where(needed, slot + 1, free)
            takes = [jnp.where(needed & (slot == k), index, take) for k, take in enumerate(takes)]
            slots.append(slot)
        for k, take in enumerate(takes):
            take_ref[k] = take
        for side in range(CORES):
            for q, first in enumerate(firsts):
                block = (plane * CORES + side + first) % blocks
                home, half = block // CORES, block % CORES
                index = (jnp.abs(home - plane) - 1) * CORES + half
                slot = 0
                for k, value in enumerate(slots):
                    slot = jnp.where(index == k, value, slot)
                inside = half + jnp.where(home == planes - 1 - plane, CORES, jnp.where(home == end, 2 * CORES, 3 * CORES))
                outside = jnp.where(inner, inside, CORES + slot)
                place_ref[side, q] = jnp.where(home == plane, half, outside)

    def choose(wave, part):
        for k in range(part * CORES, (part + 1) * CORES):
            take = take_ref[k]
            for row in range(total_x):
                value = gathered[wave][jnp.minimum(take, 2 * CORES - 1), row]
                if part:
                    value = jnp.where(take < 2 * CORES, value, far[wave][jnp.maximum(take - CORES, 0), row])
                chosen[wave][k, row] = value

    def pick(wave, step):
        other = (mate + step) % mates
        source, target = staged[wave].at[other], arrived[wave].at[mate]
        return pltpu.make_async_remote_copy(
            source, target, pick_send.at[wave, step], pick_recv.at[wave, step], device_of(other), MESH
        )

    def read_map():
        for q in range(qpoints):
            shift_ref[0, q] = map_ref[q, 0] // total_y
            shift_ref[1, q] = map_ref[q, 0] % cols_y
            if not few:
                for side in range(CORES):
                    place_ref[side, q] = (plane * CORES + side + first_block(q)) % blocks

    def stage(wave):
        size = 2 * CORES
        for q in range(qpoints):
            shift = shift_ref[0, q]
            for side in range(CORES):
                place = place_ref[side, q]
                near, last = jnp.minimum(place, size - 1), jnp.maximum(place - size, 0)
                for index in range(total_x):
                    source = wrap(shift + index, total_x)
                    if few:
                        value = jnp.where(place < size, gathered[wave][near, source], far[wave][last, source])
                    else:
                        value = gathered[wave][place, source]
                    staged[wave][index // rows_x * CORES + side, q, index % rows_x] = value
        for q in range(qpoints):
            for row in range(rows_x):
                arrived[wave][mate, q, row] = staged[wave][mate, q, row]

    def settle(wave):
        for step in range(1, mates):
            pick(wave, step).wait_recv()
        for q in range(qpoints):
            for col in range(cols_y):
                column = wrap(shift_ref[1, q] + col, cols_y)
                for part in range(parts):
                    for row in range(rows_x):
                        partner_ref[col, q, row, slab(part, wave), :] = arrived[wave][part * cols_y + column, q, row]

    def fetch(point):
        slot = point % depth
        return pltpu.make_async_copy(coupling_ref.at[:, point % rows_x, point // rows_x], held_in.at[slot], in_sem.at[slot])

    def turn(point, carry):
        slot = point % depth
        fetch(point).wait()
        turn_point(held_in.at[slot], wannier_ref[point % rows_x, point // rows_x], turned_ref.at[point // rows_x, point % rows_x])

        @pl.when(point + depth < points)
        def _():
            fetch(point + depth).start()

        return carry

    turned = 0

    def fill(count):
        nonlocal turned
        last = min(points, turned + count)
        if last > turned:
            lax.fori_loop(turned, last, turn, 0)
        turned = last

    map_copy = pltpu.make_async_copy(map_hbm, map_ref, map_sem)
    wannier_copy = pltpu.make_async_copy(wannier_hbm, wannier_ref, wannier_sem)
    wannier_copy.start()
    map_copy.start()
    for point in range(depth):
        fetch(point).start()

    has_left, has_right = plane > 0, plane < planes - 1

    barrier = pltpu.get_barrier_semaphore()
    for step in range(1, mates):
        pl.semaphore_signal(barrier, inc=1, device_id=device_of((mate + step) % mates), device_id_type=MESH)

    @pl.when(has_left)
    def _():
        pl.semaphore_signal(barrier, inc=1, device_id=(here_x, here_y - CORES), device_id_type=MESH)

    @pl.when(has_right)
    def _():
        pl.semaphore_signal(barrier, inc=1, device_id=(here_x, here_y + CORES), device_id_type=MESH)

    wannier_copy.wait()
    fill(4)
    pl.semaphore_wait(barrier, mates - 1 + has_left.astype(jnp.int32) + has_right.astype(jnp.int32))

    for wave in range(waves):
        for step in range(mates):
            spread(wave, step).start()
    map_copy.wait()
    fill(4)

    def send(wave, origin, distance, side):
        @pl.when(has_right if side else has_left)
        def _():
            chain(wave, origin, distance, side).start()

    def spread_wait(wave):
        spread(wave, 0).wait()
        for step in range(1, mates):
            spread(wave, step).wait_recv()

    def finish(wave):
        stage(wave)
        for step in range(1, mates):
            pick(wave, step).start()
        if wave > 0:
            settle(wave - 1)

    def launch(wave):
        spread_wait(wave)
        for side in range(2):
            send(wave, plane, 0, side)

    def when(condition, *calls):
        @pl.when(condition)
        def _():
            for call in calls:
                call()

    def launch_few(wave):
        spread_wait(wave)
        when(inner, hop(wave, 0).start)
        when(~inner, hop(wave, 1).start)

    read_map()
    if few:
        assign()
        for wave in range(2):
            fill(3)
            launch_few(wave)
        for tick in range(waves + 1):
            if tick < waves:
                fill(3)
                when(inner, hop(tick, 1).wait_recv, hop(tick, 2).start)
                fill(3)
                when(inner, hop(tick, 0).wait_recv, functools.partial(choose, tick, 0), hop(tick, 3).start)
                when(~inner, hop(tick, 3).wait_recv)
                if tick + 2 < waves:
                    launch_few(tick + 2)
            if tick > 0:
                wave = tick - 1
                fill(3)
                when(inner, hop(wave, 2).wait_recv, functools.partial(choose, wave, 1), hop(wave, 4).start)
                when(~inner, hop(wave, 4).wait_recv)
                finish(wave)

    for wave in range(0 if few else min(2, waves)):
        fill(3)
        launch(wave)

    for tick in range(1, 0 if few else waves + planes - 1):
        for distance in reversed(range(1, planes)):
            wave = tick - distance
            if not 0 <= wave < waves:
                continue
            fill(3)

            @pl.when(plane + distance < planes)
            def _():
                chain(wave, plane + distance, distance, 0).wait_recv()
                if distance < planes - 1:
                    send(wave, plane + distance, distance, 0)

            @pl.when(plane >= distance)
            def _():
                chain(wave, plane - distance, distance, 1).wait_recv()
                if distance < planes - 1:
                    send(wave, plane - distance, distance, 1)

        if tick + 1 < waves:
            launch(tick + 1)
        wave = tick - planes + 1
        if 0 <= wave < waves:
            finish(wave)

    fill(points)
    settle(waves - 1)

    for wave in range(waves):
        for step in range(1, mates):
            spread(wave, step).wait_send()
        if few:
            when(inner, *[hop(wave, kind).wait_send for kind in (0, 2, 3, 4)])
            when(~inner, hop(wave, 1).wait_send)
        for distance in range(0 if few else planes - 1):

            @pl.when((plane + distance < planes) & has_left)
            def _():
                chain(wave, plane + distance, distance, 0).wait_send()

            @pl.when((plane >= distance) & has_right)
            def _():
                chain(wave, plane - distance, distance, 1).wait_send()

        for step in range(1, mates):
            pick(wave, step).wait_send()


def exchange(kq_map, wannier, coupling, count_x, count_y, few):
    rows_x, cols_y, bands, width = wannier.shape
    qpoints, modes = coupling.shape[0], coupling.shape[3]
    planes, mates = count_y // CORES, count_x * CORES
    parts = mates // cols_y
    assert parts * cols_y == mates and planes * CORES == count_y
    sizes = [SLAB] * (bands // (parts * SLAB))
    slabs = [(sum(sizes[:wave]), size) for wave, size in enumerate(sizes)]
    waves = len(slabs)
    plan = (few, count_x, planes, rows_x, cols_y, qpoints, parts, slabs)

    def per_wave(*shape):
        return [pltpu.VMEM((*shape, size, width), wannier.dtype) for size in sizes]

    dma = pltpu.SemaphoreType.DMA
    hbm, vmem = pl.BlockSpec(memory_space=pltpu.HBM), pl.BlockSpec(memory_space=pltpu.VMEM)
    kind = coupling.dtype
    return pl.pallas_call(
        functools.partial(exchange_kernel, plan),
        out_shape=[
            jax.ShapeDtypeStruct((cols_y, qpoints, rows_x, bands, width), kind),
            jax.ShapeDtypeStruct((cols_y, rows_x, qpoints, 2 * bands, modes * width), kind),
        ],
        in_specs=[hbm, hbm, hbm],
        out_specs=[vmem, vmem],
        scratch_shapes=per_wave(2 * CORES if few else count_y, count_x * rows_x)
        + per_wave(2 * CORES if few else 1, count_x * rows_x)
        + per_wave(SLOTS if few else 1, count_x * rows_x)
        + per_wave(mates, qpoints, rows_x)
        + per_wave(mates, qpoints, rows_x)
        + [
            dma((waves, mates)),
            dma((waves, mates)),
            dma((waves,)),
            dma((waves, 5) if few else (waves, planes, 2)),
            dma((waves, 3) if few else (waves, planes)),
            dma((waves, mates)),
            dma((waves, mates)),
            pltpu.SMEM(kq_map.shape, jnp.int32),
            dma(()),
            pltpu.VMEM(wannier.shape, kind),
            dma(()),
            pltpu.VMEM((DEPTH, qpoints, modes, bands, width), kind),
            dma((DEPTH,)),
            pltpu.SMEM((CORES, qpoints), jnp.int32),
            pltpu.SMEM((SLOTS,), jnp.int32),
            pltpu.SMEM((2, qpoints), jnp.int32),
        ],
        compiler_params=pltpu.CompilerParams(collective_id=int(few), has_side_effects=True, vmem_limit_bytes=16 << 20),
    )(*[pltpu.with_memory_space_constraint(a, pltpu.HBM) for a in (kq_map, wannier, coupling)])


def rotate_kernel(partner_ref, turned_ref, out_hbm, out_ref, out_sem):
    cols, qpoints, rows, modes, bands, width = out_ref.shape
    half = width // 2

    def flush(col):
        return pltpu.make_async_copy(out_ref.at[col], out_hbm.at[:, :, col], out_sem.at[col])

    def one(col, carry):
        for q in range(qpoints):
            for first in range(0, rows, 2):
                partner_rows = []
                for side, row in enumerate((first, first + 1)):
                    partner = partner_ref[col, q, row]
                    column = jnp.concatenate([partner[:, :half], partner[:, half:]], axis=0)
                    blank = jnp.zeros_like(column)
                    partner_rows.append(jnp.concatenate([blank, column] if side else [column, blank], axis=1))
                rotated = lax.dot_general(
                    jnp.concatenate(partner_rows, axis=0),
                    jnp.concatenate([turned_ref[col, row, q] for row in (first, first + 1)], axis=0),
                    (((0,), (0,)), ((), ())),
                    preferred_element_type=jnp.float32,
                ).astype(out_ref.dtype)
                for side, row in enumerate((first, first + 1)):
                    for mode in range(modes):
                        out_ref[col, q, row, mode] = rotated[side * bands : (side + 1) * bands, mode * width : (mode + 1) * width]
        flush(col).start()
        return carry

    lax.fori_loop(0, cols, one, 0, unroll=UNROLL)
    for col in range(cols):
        flush(col).wait()


def rotate(turned, partner):
    cols, qpoints, rows, bands, width = partner.shape
    modes = turned.shape[-1] // width
    hbm, vmem = pl.BlockSpec(memory_space=pltpu.HBM), pl.BlockSpec(memory_space=pltpu.VMEM)
    return pl.pallas_call(
        rotate_kernel,
        in_specs=[vmem, vmem],
        out_specs=hbm,
        out_shape=pltpu.HBM((qpoints, rows, cols, modes, bands, width), turned.dtype),
        scratch_shapes=[
            pltpu.VMEM((cols, qpoints, rows, modes, bands, width), turned.dtype),
            pltpu.SemaphoreType.DMA((cols,)),
        ],
        compiler_params=pltpu.CompilerParams(vmem_limit_bytes=16 << 20),
    )(partner, turned)


def few_blocks(kq_map, cols_y, total_y, limit):
    blocks = total_y // cols_y
    kind = lax.broadcasted_iota(jnp.int32, (1, cols_y), 1)
    shift = kq_map[:, :1] % total_y
    first = ((shift - kind + cols_y - 1) // cols_y) % blocks
    count = jnp.zeros((1, cols_y), jnp.int32)
    for block in range(CORES, blocks):
        near = (first - block) % blocks
        hit = jnp.zeros((1, cols_y), bool)
        for q in range(kq_map.shape[0]):
            hit = hit | (near[q : q + 1] == 0) | (near[q : q + 1] == blocks - 1)
        count = count + hit.astype(jnp.int32)
    return jnp.max(count) <= limit


def per_device(wannier, coupling, kq_map):
    count_x, count_y = lax.axis_size("kx"), lax.axis_size("ky")

    def run(few):
        partner, turned = exchange(kq_map, wannier, coupling, count_x, count_y, few)
        return rotate(turned, partner)

    cols_y = wannier.shape[1]
    if count_y != 4 * CORES:
        return run(False)
    return lax.cond(few_blocks(kq_map, cols_y, cols_y * count_y, SLOTS), lambda: run(True), lambda: run(False))


def solution(mesh):
    in_specs = (P("kx", "ky", None, None), P(None, "kx", "ky", None, None, None), P())
    out_specs = P(None, "kx", "ky", None, None, None)
    return jax.shard_map(
        per_device, mesh=mesh, in_specs=in_specs, out_specs=out_specs, check_vma=False
    )
```

```python
import functools

import jax
import jax.numpy as jnp
from jax import lax
from jax.experimental import pallas as pl
from jax.experimental.pallas import tpu as pltpu
from jax.sharding import PartitionSpec as P

MESH = pl.DeviceIdType.MESH
CORES = 2
SLAB = 16
SLOTS = 4
UNROLL = 8
DEPTH = 4


def turn_point(coupling, wannier, out):
    qpoints, modes, bands, width = coupling.shape
    half = width // 2
    real, imag = wannier[:, :half], wannier[:, half:]
    plain = jnp.concatenate([jnp.concatenate([real, imag], axis=1), jnp.concatenate([-imag, real], axis=1)], axis=0)
    swapped = jnp.concatenate([jnp.concatenate([imag, -real], axis=1), jnp.concatenate([real, imag], axis=1)], axis=0)
    blank = jnp.zeros_like(plain)
    blocks = coupling[...].reshape(qpoints * modes // 2, 2, bands, width)
    pairs = jnp.concatenate([blocks[:, 0].reshape(-1, width), blocks[:, 1].reshape(-1, width)], axis=1)
    for side, factor in enumerate((plain, swapped)):
        pair_factor = jnp.concatenate(
            [jnp.concatenate([factor, blank], axis=1), jnp.concatenate([blank, factor], axis=1)], axis=0
        )
        turned = jnp.dot(pairs, pair_factor, preferred_element_type=jnp.float32).astype(out.dtype)
        for index in range(qpoints * modes):
            pair, lane = divmod(index, 2)
            q, mode = divmod(index, modes)
            out[q, side * bands : (side + 1) * bands, mode * width : (mode + 1) * width] = turned[
                pair * bands : (pair + 1) * bands, lane * width : (lane + 1) * width
            ]


def wrap(value, size):
    return value & (size - 1) if size & (size - 1) == 0 else lax.rem(value, size)


def exchange_kernel(plan, map_hbm, wannier_hbm, coupling_ref, partner_ref, turned_ref, *scratch):
    few, count_x, planes, rows_x, cols_y, qpoints, parts, slabs = plan
    waves = len(slabs)
    mates = count_x * CORES
    total_x, total_y, blocks = count_x * rows_x, planes * CORES * cols_y, planes * CORES
    gathered, far, chosen, staged, arrived = (scratch[part * waves : (part + 1) * waves] for part in range(5))
    spread_send, spread_recv, spread_self, chain_send, chain_recv, pick_send, pick_recv = scratch[5 * waves :][:7]
    map_ref, map_sem, wannier_ref, wannier_sem, held_in, in_sem, place_ref, take_ref, shift_ref = scratch[5 * waves + 7 :]
    points, depth = rows_x * cols_y, held_in.shape[0]

    here_x, here_y = lax.axis_index("kx"), lax.axis_index("ky")
    plane, core = here_y // CORES, here_y % CORES
    mate = here_x * CORES + core

    def device_of(other):
        return (other // CORES, plane * CORES + other % CORES)

    def part_of(other):
        return other // cols_y if parts > 1 else 0

    def slab(part, wave):
        start, size = slabs[wave]
        return pl.ds(pl.multiple_of(part * (slabs[-1][0] + slabs[-1][1]) + start, size), size)

    def spread(wave, step):
        other = (mate + step) % mates
        window = (slice(None), other % cols_y, slab(part_of(other), wave), slice(None))
        target = gathered[wave].at[core if few else here_y, pl.ds(here_x * rows_x, rows_x)]
        if step == 0:
            return pltpu.make_async_copy(wannier_hbm.at[window], target, spread_self.at[wave])
        source = wannier_ref.at[window]
        return pltpu.make_async_remote_copy(
            source, target, spread_send.at[wave, step], spread_recv.at[wave, step], device_of(other), MESH
        )

    def chain(wave, origin, distance, side):
        block = gathered[wave].at[pl.ds(origin * CORES, CORES)]
        target = (here_x, here_y + (CORES if side else -CORES))
        return pltpu.make_async_remote_copy(
            block, block, chain_send.at[wave, distance, side], chain_recv.at[wave, origin], target, MESH
        )

    inner = (plane > 0) & (plane < planes - 1)
    end = jnp.where(inner, (plane - 1) * (planes - 1), plane)

    def hop(wave, kind):
        near_pair, last_pair = pl.ds(0, CORES), pl.ds(CORES, CORES)
        other_inner, next_inner, next_end = planes - 1 - plane, 1 + plane // (planes - 1), (plane - 1) * (planes - 1)
        source, target, index, to = (
            (gathered[wave].at[near_pair], gathered[wave].at[last_pair], 0, other_inner),
            (gathered[wave].at[near_pair], far[wave].at[near_pair], 1, next_inner),
            (far[wave].at[near_pair], far[wave].at[last_pair], 2, other_inner),
            (chosen[wave].at[near_pair], gathered[wave].at[last_pair], 0, next_end),
            (chosen[wave].at[last_pair], far[wave].at[near_pair], 1, next_end),
        )[kind]
        return pltpu.make_async_remote_copy(
            source, target, chain_send.at[wave, kind], chain_recv.at[wave, index], (here_x, to * CORES + core), MESH
        )

    def first_block(q):
        return (map_ref[q, 0] % total_y - mate % cols_y + cols_y - 1) // cols_y % blocks

    def assign():
        firsts = [first_block(q) for q in range(qpoints)]
        free, slots, takes = 0, [], list(range(SLOTS))
        for index in range(blocks - CORES):
            away = index // CORES + 1
            block = jnp.where(end == 0, away, end - away) * CORES + index % CORES
            needed = False
            for first in firsts:
                ahead = (block - end * CORES - first) % blocks
                needed = needed | (ahead == 0) | (ahead == 1)
            slot = jnp.maximum(free, index - (blocks - CORES - SLOTS))
            free = jnp.where(needed, slot + 1, free)
            takes = [jnp.where(needed & (slot == k), index, take) for k, take in enumerate(takes)]
            slots.append(slot)
        for k, take in enumerate(takes):
            take_ref[k] = take
        for side in range(CORES):
            for q, first in enumerate(firsts):
                block = (plane * CORES + side + first) % blocks
                home, half = block // CORES, block % CORES
                index = (jnp.abs(home - plane) - 1) * CORES + half
                slot = 0
                for k, value in enumerate(slots):
                    slot = jnp.where(index == k, value, slot)
                inside = half + jnp.where(home == planes - 1 - plane, CORES, jnp.where(home == end, 2 * CORES, 3 * CORES))
                outside = jnp.where(inner, inside, CORES + slot)
                place_ref[side, q] = jnp.where(home == plane, half, outside)

    def choose(wave, part):
        for k in range(part * CORES, (part + 1) * CORES):
            take = take_ref[k]
            for row in range(total_x):
                value = gathered[wave][jnp.minimum(take, 2 * CORES - 1), row]
                if part:
                    value = jnp.where(take < 2 * CORES, value, far[wave][jnp.maximum(take - CORES, 0), row])
                chosen[wave][k, row] = value

    def pick(wave, step):
        other = (mate + step) % mates
        source, target = staged[wave].at[other], arrived[wave].at[mate]
        return pltpu.make_async_remote_copy(
            source, target, pick_send.at[wave, step], pick_recv.at[wave, step], device_of(other), MESH
        )

    def read_map():
        for q in range(qpoints):
            shift_ref[0, q] = map_ref[q, 0] // total_y
            shift_ref[1, q] = map_ref[q, 0] % cols_y
            if not few:
                for side in range(CORES):
                    place_ref[side, q] = (plane * CORES + side + first_block(q)) % blocks

    def stage(wave):
        size = 2 * CORES
        for q in range(qpoints):
            shift = shift_ref[0, q]
            for side in range(CORES):
                place = place_ref[side, q]
                near, last = jnp.minimum(place, size - 1), jnp.maximum(place - size, 0)
                for index in range(total_x):
                    source = wrap(shift + index, total_x)
                    if few:
                        value = jnp.where(place < size, gathered[wave][near, source], far[wave][last, source])
                    else:
                        value = gathered[wave][place, source]
                    staged[wave][index // rows_x * CORES + side, q, index % rows_x] = value
        for q in range(qpoints):
            for row in range(rows_x):
                arrived[wave][mate, q, row] = staged[wave][mate, q, row]

    def settle(wave):
        for step in range(1, mates):
            pick(wave, step).wait_recv()
        for q in range(qpoints):
            for col in range(cols_y):
                column = wrap(shift_ref[1, q] + col, cols_y)
                for part in range(parts):
                    for row in range(rows_x):
                        partner_ref[col, q, row, slab(part, wave), :] = arrived[wave][part * cols_y + column, q, row]

    def fetch(point):
        slot = point % depth
        return pltpu.make_async_copy(coupling_ref.at[:, point % rows_x, point // rows_x], held_in.at[slot], in_sem.at[slot])

    def turn(point, carry):
        slot = point % depth
        fetch(point).wait()
        turn_point(held_in.at[slot], wannier_ref[point % rows_x, point // rows_x], turned_ref.at[point // rows_x, point % rows_x])

        @pl.when(point + depth < points)
        def _():
            fetch(point + depth).start()

        return carry

    turned = 0

    def fill(count):
        nonlocal turned
        last = min(points, turned + count)
        if last > turned:
            lax.fori_loop(turned, last, turn, 0)
        turned = last

    map_copy = pltpu.make_async_copy(map_hbm, map_ref, map_sem)
    wannier_copy = pltpu.make_async_copy(wannier_hbm, wannier_ref, wannier_sem)
    wannier_copy.start()
    map_copy.start()
    for point in range(depth):
        fetch(point).start()

    has_left, has_right = plane > 0, plane < planes - 1

    barrier = pltpu.get_barrier_semaphore()
    for step in range(1, mates):
        pl.semaphore_signal(barrier, inc=1, device_id=device_of((mate + step) % mates), device_id_type=MESH)

    @pl.when(has_left)
    def _():
        pl.semaphore_signal(barrier, inc=1, device_id=(here_x, here_y - CORES), device_id_type=MESH)

    @pl.when(has_right)
    def _():
        pl.semaphore_signal(barrier, inc=1, device_id=(here_x, here_y + CORES), device_id_type=MESH)

    wannier_copy.wait()
    pl.semaphore_wait(barrier, mates - 1 + has_left.astype(jnp.int32) + has_right.astype(jnp.int32))

    for wave in range(waves):
        for step in range(mates):
            spread(wave, step).start()
    map_copy.wait()
    fill(6)

    def send(wave, origin, distance, side):
        @pl.when(has_right if side else has_left)
        def _():
            chain(wave, origin, distance, side).start()

    def spread_wait(wave):
        spread(wave, 0).wait()
        for step in range(1, mates):
            spread(wave, step).wait_recv()

    def finish(wave):
        stage(wave)
        for step in range(1, mates):
            pick(wave, step).start()
        if wave > 1:
            settle(wave - 2)

    def launch(wave):
        spread_wait(wave)
        for side in range(2):
            send(wave, plane, 0, side)

    def when(condition, *calls):
        @pl.when(condition)
        def _():
            for call in calls:
                call()

    def launch_few(wave):
        spread_wait(wave)
        when(inner, hop(wave, 0).start)
        when(~inner, hop(wave, 1).start)

    read_map()
    if few:
        assign()
        for wave in range(2):
            fill(3)
            launch_few(wave)
        for tick in range(waves + 1):
            if tick < waves:
                fill(3)
                when(inner, hop(tick, 1).wait_recv, hop(tick, 2).start)
                fill(3)
                when(inner, hop(tick, 0).wait_recv, functools.partial(choose, tick, 0), hop(tick, 3).start)
                when(~inner, hop(tick, 3).wait_recv)
                if tick + 2 < waves:
                    launch_few(tick + 2)
            if tick > 0:
                wave = tick - 1
                fill(3)
                when(inner, hop(wave, 2).wait_recv, functools.partial(choose, wave, 1), hop(wave, 4).start)
                when(~inner, hop(wave, 4).wait_recv)
                finish(wave)

    for wave in range(0 if few else min(2, waves)):
        fill(3)
        launch(wave)

    for tick in range(1, 0 if few else waves + planes - 1):
        for distance in reversed(range(1, planes)):
            wave = tick - distance
            if not 0 <= wave < waves:
                continue
            fill(3)

            @pl.when(plane + distance < planes)
            def _():
                chain(wave, plane + distance, distance, 0).wait_recv()
                if distance < planes - 1:
                    send(wave, plane + distance, distance, 0)

            @pl.when(plane >= distance)
            def _():
                chain(wave, plane - distance, distance, 1).wait_recv()
                if distance < planes - 1:
                    send(wave, plane - distance, distance, 1)

        if tick + 1 < waves:
            launch(tick + 1)
        wave = tick - planes + 1
        if 0 <= wave < waves:
            finish(wave)

    fill(points)
    for wave in range(max(0, waves - 2), waves):
        settle(wave)

    for wave in range(waves):
        for step in range(1, mates):
            spread(wave, step).wait_send()
        if few:
            when(inner, *[hop(wave, kind).wait_send for kind in (0, 2, 3, 4)])
            when(~inner, hop(wave, 1).wait_send)
        for distance in range(0 if few else planes - 1):

            @pl.when((plane + distance < planes) & has_left)
            def _():
                chain(wave, plane + distance, distance, 0).wait_send()

            @pl.when((plane >= distance) & has_right)
            def _():
                chain(wave, plane - distance, distance, 1).wait_send()

        for step in range(1, mates):
            pick(wave, step).wait_send()


def exchange(kq_map, wannier, coupling, count_x, count_y, few):
    rows_x, cols_y, bands, width = wannier.shape
    qpoints, modes = coupling.shape[0], coupling.shape[3]
    planes, mates = count_y // CORES, count_x * CORES
    parts = mates // cols_y
    assert parts * cols_y == mates and planes * CORES == count_y
    sizes = [SLAB] * (bands // (parts * SLAB))
    slabs = [(sum(sizes[:wave]), size) for wave, size in enumerate(sizes)]
    waves = len(slabs)
    plan = (few, count_x, planes, rows_x, cols_y, qpoints, parts, slabs)

    def per_wave(*shape):
        return [pltpu.VMEM((*shape, size, width), wannier.dtype) for size in sizes]

    dma = pltpu.SemaphoreType.DMA
    hbm, vmem = pl.BlockSpec(memory_space=pltpu.HBM), pl.BlockSpec(memory_space=pltpu.VMEM)
    kind = coupling.dtype
    return pl.pallas_call(
        functools.partial(exchange_kernel, plan),
        out_shape=[
            jax.ShapeDtypeStruct((cols_y, qpoints, rows_x, bands, width), kind),
            jax.ShapeDtypeStruct((cols_y, rows_x, qpoints, 2 * bands, modes * width), kind),
        ],
        in_specs=[hbm, hbm, hbm],
        out_specs=[vmem, vmem],
        scratch_shapes=per_wave(2 * CORES if few else count_y, count_x * rows_x)
        + per_wave(2 * CORES if few else 1, count_x * rows_x)
        + per_wave(SLOTS if few else 1, count_x * rows_x)
        + per_wave(mates, qpoints, rows_x)
        + per_wave(mates, qpoints, rows_x)
        + [
            dma((waves, mates)),
            dma((waves, mates)),
            dma((waves,)),
            dma((waves, 5) if few else (waves, planes, 2)),
            dma((waves, 3) if few else (waves, planes)),
            dma((waves, mates)),
            dma((waves, mates)),
            pltpu.SMEM(kq_map.shape, jnp.int32),
            dma(()),
            pltpu.VMEM(wannier.shape, kind),
            dma(()),
            pltpu.VMEM((DEPTH, qpoints, modes, bands, width), kind),
            dma((DEPTH,)),
            pltpu.SMEM((CORES, qpoints), jnp.int32),
            pltpu.SMEM((SLOTS,), jnp.int32),
            pltpu.SMEM((2, qpoints), jnp.int32),
        ],
        compiler_params=pltpu.CompilerParams(collective_id=int(few), has_side_effects=True, vmem_limit_bytes=16 << 20),
    )(*[pltpu.with_memory_space_constraint(a, pltpu.HBM) for a in (kq_map, wannier, coupling)])


def rotate_kernel(partner_ref, turned_ref, out_hbm, out_ref, out_sem):
    cols, qpoints, rows, modes, bands, width = out_ref.shape
    half = width // 2

    def flush(col, q):
        return pltpu.make_async_copy(out_ref.at[col, q], out_hbm.at[q, :, col], out_sem.at[col, q])

    def one(col, carry):
        for q in range(qpoints):
            for first in range(0, rows, 2):
                partner_rows = []
                for side, row in enumerate((first, first + 1)):
                    partner = partner_ref[col, q, row]
                    column = jnp.concatenate([partner[:, :half], partner[:, half:]], axis=0)
                    blank = jnp.zeros_like(column)
                    partner_rows.append(jnp.concatenate([blank, column] if side else [column, blank], axis=1))
                rotated = lax.dot_general(
                    jnp.concatenate(partner_rows, axis=0),
                    jnp.concatenate([turned_ref[col, row, q] for row in (first, first + 1)], axis=0),
                    (((0,), (0,)), ((), ())),
                    preferred_element_type=jnp.float32,
                ).astype(out_ref.dtype)
                for side, row in enumerate((first, first + 1)):
                    for mode in range(modes):
                        out_ref[col, q, row, mode] = rotated[side * bands : (side + 1) * bands, mode * width : (mode + 1) * width]
            flush(col, q).start()
        return carry

    lax.fori_loop(0, cols, one, 0, unroll=UNROLL)
    for col in range(cols):
        for q in range(qpoints):
            flush(col, q).wait()


def rotate(turned, partner):
    cols, qpoints, rows, bands, width = partner.shape
    modes = turned.shape[-1] // width
    hbm, vmem = pl.BlockSpec(memory_space=pltpu.HBM), pl.BlockSpec(memory_space=pltpu.VMEM)
    return pl.pallas_call(
        rotate_kernel,
        in_specs=[vmem, vmem],
        out_specs=hbm,
        out_shape=pltpu.HBM((qpoints, rows, cols, modes, bands, width), turned.dtype),
        scratch_shapes=[
            pltpu.VMEM((cols, qpoints, rows, modes, bands, width), turned.dtype),
            pltpu.SemaphoreType.DMA((cols, qpoints)),
        ],
        compiler_params=pltpu.CompilerParams(vmem_limit_bytes=16 << 20),
    )(partner, turned)


def few_blocks(kq_map, cols_y, total_y, limit):
    blocks = total_y // cols_y
    kind = lax.broadcasted_iota(jnp.int32, (1, cols_y), 1)
    first = (kq_map[:, :1] - kind + cols_y - 1) // cols_y % blocks
    needed = lax.reduce((1 << first) | (1 << (first + 1) % blocks), 0, lax.bitwise_or, (0,))
    return jnp.max(lax.population_count(needed >> CORES)) <= limit


def per_device(wannier, coupling, kq_map):
    count_x, count_y = lax.axis_size("kx"), lax.axis_size("ky")

    def run(few):
        partner, turned = exchange(kq_map, wannier, coupling, count_x, count_y, few)
        return rotate(turned, partner)

    cols_y = wannier.shape[1]
    if count_y != 4 * CORES:
        return run(False)
    return lax.cond(few_blocks(kq_map, cols_y, cols_y * count_y, SLOTS), lambda: run(True), lambda: run(False))


def solution(mesh):
    in_specs = (P("kx", "ky", None, None), P(None, "kx", "ky", None, None, None), P())
    out_specs = P(None, "kx", "ky", None, None, None)
    return jax.shard_map(
        per_device, mesh=mesh, in_specs=in_specs, out_specs=out_specs, check_vma=False
    )
```
